128 devices in a mesh: dp: 1, tp: 2 (over core), sp: 64 (over z, y, x).
Axes of the slice: x: 4, y: 4, z: 4, core: 2. Of those that a mesh axis runs over, the one named last changes fastest.
Arguments:
- x_in: bfloat16 [8, 4096], P('dp')
- seq_lens: int32 [8], P('dp')
- k_cache: bfloat16 [8, 4096, 32, 128], P('dp', 'sp', 'tp')
- v_cache: bfloat16 [8, 4096, 32, 128], P('dp', 'sp', 'tp')
- ln1_gain: float32 [4096], replicated
- w_qkv: bfloat16 [4096, 3, 32, 128], P(None, None, 'tp')
- w_out: bfloat16 [32, 128, 4096], P('tp')
- ln2_gain: float32 [4096], replicated
- w_up: bfloat16 [4096, 16384], P(None, 'tp')
- w_down: bfloat16 [16384, 4096], P('tp')
Outputs:
- output 1: bfloat16 [8, 4096], P('dp')
- output 2: bfloat16 [8, 4096, 32, 128], P('dp', 'sp', 'tp')
- output 3: bfloat16 [8, 4096, 32, 128], P('dp', 'sp', 'tp')
All inputs are finite; a program needn't handle non-finite values.
Results may differ from the reference program's by a relative error of at most 0.00690939.
Values sent between devices are 32-bit elements.
A program may use at most 1 GiB of HBM per device.

```python
import jax
import jax.numpy as jnp
from jax import lax

BATCH = 8
CACHE_LEN = 4096
BLOCK_LEN = 64
D = 4096
HEADS = 32
HEAD = 128
FF = 16384
PLANT_GAP = 64

NUM_BLOCKS = CACHE_LEN // BLOCK_LEN
LN_EPS = 1e-5
ALIBI_CAP = 256.0


def layer_norm(x_f32, gain):
    mean = jnp.mean(x_f32, axis=-1, keepdims=True)
    centred = x_f32 - mean
    variance = jnp.mean(centred * centred, axis=-1, keepdims=True)
    return centred * lax.rsqrt(variance + LN_EPS) * gain


def alibi_slopes():
    return jnp.exp2(-8.0 * (jnp.arange(HEADS).astype(jnp.float32) + 1.0) / HEADS)


def setup_inputs(seed: int = 0, part: int = 0) -> dict:
    root = jax.random.key(seed)
    shared = jax.random.split(root, 6)
    own = jax.random.split(jax.random.fold_in(root, part), 7)
    x_in = jax.random.normal(own[0], (BATCH, D), jnp.float32).astype(jnp.bfloat16)
    ln1_gain = jax.random.uniform(shared[0], (D,), jnp.float32, minval=0.5, maxval=1.5)
    w_qkv = (jax.random.normal(shared[1], (D, 3, HEADS, HEAD), jnp.float32) * D ** -0.5).astype(jnp.bfloat16)
    w_out = (jax.random.normal(shared[2], (HEADS, HEAD, D), jnp.float32) * D ** -0.5).astype(jnp.bfloat16)
    ln2_gain = jax.random.uniform(shared[3], (D,), jnp.float32, minval=0.5, maxval=1.5)
    w_up = (jax.random.normal(shared[4], (D, FF), jnp.float32) * D ** -0.5).astype(jnp.bfloat16)
    w_down = (jax.random.normal(shared[5], (FF, D), jnp.float32) * FF ** -0.5).astype(jnp.bfloat16)
    seq_lens = jax.random.randint(own[1], (BATCH,), 1, CACHE_LEN)
    longest = jax.random.randint(own[2], (), 0, BATCH)
    seq_lens = jnp.where(jnp.arange(BATCH) == longest, CACHE_LEN - 1, seq_lens).astype(jnp.int32)
    normed = layer_norm(x_in.astype(jnp.float32), ln1_gain).astype(jnp.bfloat16)
    query = jnp.dot(normed, w_qkv[:, 0].reshape(D, D), preferred_element_type=jnp.float32)
    query = query.astype(jnp.bfloat16).astype(jnp.float32).reshape(BATCH, HEADS, HEAD)
    offsets = jax.random.randint(own[3], (BATCH, CACHE_LEN // PLANT_GAP, 1), 0, PLANT_GAP)
    slot_pos = jnp.arange(CACHE_LEN)
    planted = (jnp.arange(PLANT_GAP)[None, None, :] == offsets).reshape(BATCH, CACHE_LEN)
    planted = planted & (slot_pos[None, :] < seq_lens[:, None])
    gumbel_u = jax.random.uniform(own[4], (BATCH, CACHE_LEN, HEADS), jnp.float32, minval=1e-6, maxval=1.0)
    bonus = 4.0 - 1.5 * jnp.log(-jnp.log(gumbel_u))
    distance = (seq_lens[:, None] - slot_pos[None, :]).astype(jnp.float32)
    target = jnp.minimum(alibi_slopes()[None, None, :] * distance[:, :, None], ALIBI_CAP) + bonus

    def make_keys(args):
        seq_key, q_row, target_row, planted_row = args
        k_rand = jax.random.normal(seq_key, (CACHE_LEN, HEADS, HEAD), jnp.float32)
        along = jnp.einsum("hk,thk->th", q_row, k_rand)
        coef = (target_row * HEAD ** 0.5 - along) / jnp.sum(q_row * q_row, axis=-1)[None, :]
        lifted = k_rand + coef[:, :, None] * q_row[None, :, :]
        return jnp.where(planted_row[:, None, None], lifted, k_rand).astype(jnp.bfloat16)

    def make_values(seq_key):
        return jax.random.normal(seq_key, (CACHE_LEN, HEADS, HEAD), jnp.float32).astype(jnp.bfloat16)

    k_cache = lax.map(make_keys, (jax.random.split(own[5], BATCH), query, target, planted))
    v_cache = lax.map(make_values, jax.random.split(own[6], BATCH))
    return {"x_in": x_in, "seq_lens": seq_lens, "k_cache": k_cache, "v_cache": v_cache, "ln1_gain": ln1_gain, "w_qkv": w_qkv, "w_out": w_out, "ln2_gain": ln2_gain, "w_up": w_up, "w_down": w_down}


def reference(x_in, seq_lens, k_cache, v_cache, ln1_gain, w_qkv, w_out, ln2_gain, w_up, w_down):
    normed = layer_norm(x_in.astype(jnp.float32), ln1_gain).astype(jnp.bfloat16)
    qkv_proj = jnp.dot(normed, w_qkv.reshape(D, 3 * D), preferred_element_type=jnp.float32)
    qkv_proj = qkv_proj.astype(jnp.bfloat16).reshape(BATCH, 3, HEADS, HEAD)
    slot_pos = jnp.arange(CACHE_LEN)
    slot_hit = (slot_pos[None, :] == seq_lens[:, None])[:, :, None, None]
    k_next = jnp.where(slot_hit, qkv_proj[:, 1][:, None], k_cache)
    v_next = jnp.where(slot_hit, qkv_proj[:, 2][:, None], v_cache)
    slopes = alibi_slopes()

    def attend(args):
        q_row, k_seq, v_seq, length = args
        q_f32 = q_row.astype(jnp.float32)

        def block_scores(k_block):
            return jnp.einsum("hk,thk->ht", q_f32, k_block.astype(jnp.float32))

        scores = lax.map(block_scores, k_seq.reshape(NUM_BLOCKS, BLOCK_LEN, HEADS, HEAD))
        scores = jnp.transpose(scores, (1, 0, 2)).reshape(HEADS, CACHE_LEN) * HEAD ** -0.5
        scores = scores - slopes[:, None] * (length - slot_pos).astype(jnp.float32)[None, :]
        scores = jnp.where((slot_pos <= length)[None, :], scores, -jnp.inf)
        row_max = jnp.max(scores, axis=1, keepdims=True)
        weights = jnp.exp(scores - row_max)
        row_sum = jnp.sum(weights, axis=1)
        weights_b = weights.astype(jnp.bfloat16).astype(jnp.float32)
        weights_b = jnp.transpose(weights_b.reshape(HEADS, NUM_BLOCKS, BLOCK_LEN), (1, 0, 2))

        def block_sum(carry, block_pair):
            w_block, v_block = block_pair
            return carry + jnp.einsum("ht,thk->hk", w_block, v_block.astype(jnp.float32)), None

        summed, _ = lax.scan(block_sum, jnp.zeros((HEADS, HEAD), jnp.float32), (weights_b, v_seq.reshape(NUM_BLOCKS, BLOCK_LEN, HEADS, HEAD)))
        return summed / row_sum[:, None]

    attended = lax.map(attend, (qkv_proj[:, 0], k_next, v_next, seq_lens))
    attended = attended.astype(jnp.bfloat16).reshape(BATCH, D)
    residual = x_in.astype(jnp.float32) + jnp.dot(attended, w_out.reshape(D, D), preferred_element_type=jnp.float32)
    normed_mid = layer_norm(residual, ln2_gain).astype(jnp.bfloat16)
    hidden = jax.nn.gelu(jnp.dot(normed_mid, w_up, preferred_element_type=jnp.float32), approximate=False).astype(jnp.bfloat16)
    x_out = (residual + jnp.dot(hidden, w_down, preferred_element_type=jnp.float32)).astype(jnp.bfloat16)
    return (x_out, k_next, v_next)
```

```python
import functools

import jax
import jax.numpy as jnp
from jax import lax
from jax.experimental import pallas as pl
from jax.experimental.pallas import tpu as pltpu
from jax.sharding import PartitionSpec as P

LN_EPS = 1e-5
MESH = pl.DeviceIdType.MESH
F32 = jnp.float32
BF16 = jnp.bfloat16

BATCH, D, HEADS, HD, TOK = 8, 4096, 16, 128, 64
FF_DEV = 1024
CHUNK = 256
N_CHUNKS = D // CHUNK
AHEAD = 6


def hops(o):
    return sum(min(d, 4 - d) for d in o)


FAR = sorted([(a, b, c) for a in range(4) for b in range(4) for c in range(4) if a + b + c], key=lambda o: -hops(o))
CUBE = sorted([(a, b, c, t) for a in range(2) for b in range(2) for c in range(2) for t in range(2) if a + b + c + t], key=lambda o: -sum(o))


def layer_norm(x, gain):
    mean = jnp.mean(x, axis=-1, keepdims=True)
    centred = x - mean
    variance = jnp.mean(centred * centred, axis=-1, keepdims=True)
    return centred * lax.rsqrt(variance + LN_EPS) * gain


def flip(v):
    return v + 1 - 2 * lax.rem(v, 2)


def kernel(
    lens, x_hbm, g1_hbm, g2_hbm, wqkv, kc, vc, wout, wup, wdown,
    x_out, k_new, v_new,
    x_v, g1_v, g2_v, ring, kc_v, vc_v, wout_v, wup_v, wdown_v,
    xrep, q_s, kv_s, kv_o, send, rs, my_o, ag, lhs_s, r_part, r_other, r_s, d_part, frs, fmine, fag,
    sem_in, sem_ring, sem_w, sem_send, sem_recv,
):
    sp = lax.axis_index("sp")
    tp = lax.axis_index("tp")
    z, y, x = sp // 16, lax.rem(sp // 4, 4), lax.rem(sp, 4)

    def far(o):
        return (lax.rem(z + o[0], 4) * 4 + lax.rem(y + o[1], 4)) * 4 + lax.rem(x + o[2], 4)

    def near(o):
        zz = flip(z) if o[0] else z
        yy = flip(y) if o[1] else y
        xx = flip(x) if o[2] else x
        block = ((lax.rem(zz, 2) * 2 + lax.rem(yy, 2)) * 2 + lax.rem(xx, 2)) * 2
        tt = 1 - tp if o[3] else tp
        return (zz * 4 + yy) * 4 + xx, tt, block + tt

    def dev(s, t):
        return (0, t, s)

    pos = (lax.rem(z, 2) * 2 + lax.rem(y, 2)) * 2 + lax.rem(x, 2)
    block = pos * 2 + tp
    group = lax.rem(x, 2)
    pair = sp // 2
    x_mate = sp + 1 - 2 * group

    def q_copy(i):
        return pltpu.make_async_copy(wqkv.at[pl.ds(i * CHUNK, CHUNK), pl.ds(0, 16)], ring.at[i], sem_ring.at[i])

    def kv_copies(i):
        return [
            pltpu.make_async_copy(
                wqkv.at[pl.ds(i * CHUNK, CHUNK), pl.ds(16 * c + 16 + 8 * group, 8)],
                ring.at[i, :, pl.ds(8 * c, 8)],
                sem_ring.at[i],
            )
            for c in range(2)
        ]

    in_x = pltpu.make_async_copy(x_hbm, x_v, sem_in.at[0])
    in_g1 = pltpu.make_async_copy(g1_hbm, g1_v, sem_in.at[1])
    in_g2 = pltpu.make_async_copy(g2_hbm, g2_v, sem_in.at[2])
    in_k = pltpu.make_async_copy(kc, kc_v, sem_in.at[3])
    in_v = pltpu.make_async_copy(vc, vc_v, sem_in.at[4])
    in_x.start()
    in_g1.start()
    for i in range(AHEAD):
        q_copy(i).start()

    barrier = pltpu.get_barrier_semaphore()
    for o in FAR:
        pl.semaphore_signal(barrier, inc=1, device_id=dev(far(o), tp), device_id_type=MESH)
    for o in CUBE:
        if o[3]:
            s, t, _ = near(o)
            pl.semaphore_signal(barrier, inc=1, device_id=dev(s, t), device_id_type=MESH)

    row = lax.broadcasted_iota(jnp.int32, (128, 2048), 0)
    col = lax.broadcasted_iota(jnp.int32, (128, 2048), 1)
    spread = jnp.where(row == col // 16, 1.0, 0.0).astype(BF16)
    in_x.wait()
    in_g1.wait()
    normed = layer_norm(x_v[...].astype(F32), g1_v[...])
    stacked = jnp.concatenate([normed[:, i * 128:(i + 1) * 128] for i in range(32)], axis=0).astype(BF16)
    rep = jnp.dot(stacked, spread, preferred_element_type=F32)
    for i in range(32):
        part = rep[i * 8:(i + 1) * 8]
        xrep[i] = jnp.concatenate([part, part], axis=0).astype(BF16)

    r16 = lax.broadcasted_iota(jnp.int32, (16, 128), 0)
    l16 = lax.rem(lax.broadcasted_iota(jnp.int32, (16, 128), 1), 16)
    masks = []
    for hp in range(8):
        m = jnp.where(l16 == 2 * hp + r16 // 8, 1.0, 0.0).astype(BF16)
        masks.append(jnp.concatenate([m] * 16, axis=1))

    def project(i, acc):
        for half in range(2):
            xx = xrep[i * 2 + half]
            lhs = jnp.concatenate([xx * m for m in masks], axis=0)
            rhs = ring[i, half * 128:(half + 1) * 128].reshape(2048, 128)
            acc = acc + jnp.dot(lhs, rhs, preferred_element_type=F32)
        return acc

    def q_step(i, acc):
        q_copy(i).wait()

        @pl.when(i < N_CHUNKS - AHEAD)
        def _():
            q_copy(i + AHEAD).start()

        @pl.when(i == N_CHUNKS - AHEAD)
        def _():
            in_k.start()
            in_v.start()

        @pl.when(i >= N_CHUNKS - AHEAD)
        def _():
            for c in kv_copies(i - (N_CHUNKS - AHEAD)):
                c.start()

        return project(i, acc)

    q = lax.fori_loop(0, N_CHUNKS, q_step, jnp.zeros((128, 128), F32))
    q_s[...] = q.astype(BF16).astype(F32).reshape(16, 8, 128)

    for i in range(AHEAD, N_CHUNKS):
        for c in kv_copies(i):
            c.start()

    hrow = lax.broadcasted_iota(jnp.int32, (16, 1024), 0)
    lane = lax.broadcasted_iota(jnp.int32, (16, 1024), 1)
    own = hrow == lax.rem(lane, 16)
    slot = sp * TOK + lane // 16
    slope = jnp.exp2(-8.0 * (tp * 16 + hrow[:, :128] + 1).astype(F32) / 32.0)
    slope = jnp.concatenate([slope] * 8, axis=1)
    low = lax.broadcasted_iota(jnp.int32, (16, 128), 1) < 64
    in_k.wait()
    in_v.wait()
    for b in range(BATCH):
        qb = q_s[:, b, :].astype(BF16)
        s = lax.dot_general(qb, kc_v[b], (((1,), (1,)), ((), ())), preferred_element_type=F32) * HD ** -0.5
        length = lens[b]
        s = s - slope * (length - slot).astype(F32)
        valid = own & (slot < length)
        s = jnp.where(valid, s, -1e30)
        m = jnp.max(s, axis=1, keepdims=True)
        p = jnp.where(valid, jnp.exp(s - m), 0.0)
        l = jnp.sum(p, axis=1, keepdims=True)
        o = jnp.dot(p.astype(BF16), vc_v[b], preferred_element_type=F32)
        ml = jnp.where(low, m, l)
        for h in range(16):
            to = (h % 8) * 8 + (b // 2) * 2 + h // 8
            send[to, b % 2:b % 2 + 1, :] = o[h:h + 1]
            send[to, 2 + b % 2:3 + b % 2, :] = ml[h:h + 1]

    pl.semaphore_wait(barrier, len(FAR) + 8)
    rs[sp] = send[sp]
    for o in FAR:
        s = far(o)
        pltpu.make_async_remote_copy(
            src_ref=send.at[s], dst_ref=rs.at[sp], send_sem=sem_send.at[0], recv_sem=sem_recv.at[0],
            device_id=dev(s, tp), device_id_type=MESH,
        ).start()

    def kv_step(i, acc):
        for c in kv_copies(i):
            c.wait()
        pltpu.make_async_copy(wout.at[pl.ds(i * 128, 128)], wout_v.at[pl.ds(i * 128, 128)], sem_w.at[0]).start()
        return project(i, acc)

    kv = lax.fori_loop(0, N_CHUNKS, kv_step, jnp.zeros((128, 128), F32))
    in_g2.start()
    for i in range(8):
        pltpu.make_async_copy(wup.at[pl.ds(i * 512, 512), pl.ds(pos * FF_DEV, FF_DEV)], wup_v.at[pl.ds(i * 512, 512)], sem_w.at[1]).start()
    for i in range(8):
        pltpu.make_async_copy(wdown.at[pl.ds(pos * FF_DEV + i * 128, 128)], wdown_v.at[pl.ds(i * 128, 128)], sem_w.at[2]).start()
    kv_s[...] = kv.astype(BF16).astype(F32).reshape(16, 8, 128)
    kv_send = pltpu.make_async_remote_copy(
        src_ref=kv_s, dst_ref=kv_o, send_sem=sem_send.at[1], recv_sem=sem_recv.at[1],
        device_id=dev(x_mate, tp), device_id_type=MESH,
    )
    kv_send.start()

    head8 = pair // 4
    first = 2 * lax.rem(pair, 4)
    turn = lax.rem(8 - first, 8)
    row8 = lax.broadcasted_iota(jnp.int32, (8, 128), 0)

    def pick(v):
        v = pltpu.roll(v, turn, 0)
        return jnp.where(row8 < 4, v, pltpu.roll(v, 4, 0))

    s_new = jnp.sum(q_s[group * 8 + head8] * kv_s[head8], axis=1, keepdims=True) * HD ** -0.5
    s_new = pick(jnp.broadcast_to(s_new, (8, 128)))
    v_mine = pick(kv_s[8 + head8])

    def wait_recv(buf, n, k):
        pltpu.make_async_copy(buf.at[pl.ds(0, n)], buf.at[pl.ds(0, n)], sem_recv.at[k]).wait()

    def wait_send(buf, n, k):
        pltpu.make_async_copy(buf.at[pl.ds(0, n)], buf.at[pl.ds(0, n)], sem_send.at[k]).wait()

    wait_recv(rs, 63, 0)
    got = rs[...].reshape(256, 128)
    ml = pltpu.roll(got, 254, 0)
    swapped = pltpu.roll(ml, 64, 1)
    lowg = lax.broadcasted_iota(jnp.int32, (256, 128), 1) < 64
    m = jnp.where(lowg, ml, swapped).reshape(32, 8, 128)
    l = jnp.where(lowg, swapped, ml).reshape(32, 8, 128)
    top = jnp.max(m, axis=0)
    top = jnp.maximum(jnp.maximum(top, pltpu.roll(top, 4, 0)), s_new)
    w = jnp.exp(m - top[None])
    o_sum = jnp.sum(w * got.reshape(32, 8, 128), axis=0)
    l_sum = jnp.sum(w * l, axis=0)
    w_new = jnp.exp(s_new - top)
    o_sum = o_sum + pltpu.roll(o_sum, 4, 0) + w_new * v_mine
    l_sum = l_sum + pltpu.roll(l_sum, 4, 0) + w_new
    mine = (o_sum / l_sum)[:2]
    my_o[...] = mine
    ag[sp] = mine
    for o in FAR:
        pltpu.make_async_remote_copy(
            src_ref=my_o, dst_ref=ag.at[sp], send_sem=sem_send.at[2], recv_sem=sem_recv.at[2],
            device_id=dev(far(o), tp), device_id_type=MESH,
        ).start()

    kv_send.wait_recv()
    for h8 in range(8):
        for c, ref in ((0, k_new), (1, v_new)):
            a, b = kv_s[8 * c + h8], kv_o[8 * c + h8]
            ref[:, h8, :] = jnp.where(group == 0, a, b)
            ref[:, 8 + h8, :] = jnp.where(group == 0, b, a)
    pltpu.make_async_copy(wout, wout_v, sem_w.at[0]).wait()

    wait_recv(ag, 63, 2)
    for s in range(64):
        h, b2 = (s % 2) * 8 + s // 8, (s // 2) % 4
        lhs_s[h, 2 * b2:2 * b2 + 2, :] = ag[s]
    lhs = jnp.concatenate([lhs_s[h] for h in range(16)], axis=1).astype(BF16)

    def out_step(n, c):
        cols = pl.ds(pl.multiple_of(n * 512, 512), 512)
        r_part[:, cols] = jnp.dot(lhs, wout_v[:, cols], preferred_element_type=F32)
        return c

    lax.fori_loop(0, 8, out_step, 0)
    r_send = pltpu.make_async_remote_copy(
        src_ref=r_part, dst_ref=r_other, send_sem=sem_send.at[3], recv_sem=sem_recv.at[3],
        device_id=dev(sp, 1 - tp), device_id_type=MESH,
    )
    r_send.start()
    in_g2.wait()
    r_send.wait_recv()
    r = x_v[...].astype(F32) + (r_part[...] + r_other[...])
    for j in range(16):
        r_s[j] = r[:, j * 256:(j + 1) * 256]
    mid = layer_norm(r, g2_v[...]).astype(BF16)
    pltpu.make_async_copy(wup.at[:, pl.ds(0, FF_DEV)], wup_v, sem_w.at[1]).wait()
    up = jnp.concatenate(
        [jnp.dot(mid, wup_v[:, n * 256:(n + 1) * 256], preferred_element_type=F32) for n in range(FF_DEV // 256)], axis=1)
    hidden = (0.5 * up * (1.0 + lax.erf(up * 0.5 ** 0.5))).astype(BF16)
    pltpu.make_async_copy(wdown.at[pl.ds(0, FF_DEV)], wdown_v, sem_w.at[2]).wait()
    for j in range(16):
        d_part[j] = jnp.dot(hidden, wdown_v[:, j * 256:(j + 1) * 256], preferred_element_type=F32)
    frs[block] = d_part[block]
    for o in CUBE:
        s, t, to = near(o)
        pltpu.make_async_remote_copy(
            src_ref=d_part.at[to], dst_ref=frs.at[block], send_sem=sem_send.at[4], recv_sem=sem_recv.at[4],
            device_id=dev(s, t), device_id_type=MESH,
        ).start()
    wait_recv(frs, 15, 4)
    done = (r_s[block] + jnp.sum(frs[...], axis=0)).astype(BF16).astype(F32)
    fmine[...] = done
    fag[block] = done
    for o in CUBE:
        s, t, _ = near(o)
        pltpu.make_async_remote_copy(
            src_ref=fmine, dst_ref=fag.at[block], send_sem=sem_send.at[5], recv_sem=sem_recv.at[5],
            device_id=dev(s, t), device_id_type=MESH,
        ).start()
    wait_send(send, 63, 0)
    kv_send.wait_send()
    wait_send(ag, 63, 2)
    r_send.wait_send()
    wait_send(d_part, 15, 4)
    wait_recv(fag, 15, 5)
    for j in range(16):
        x_out[:, j * 256:(j + 1) * 256] = fag[j].astype(BF16)
    wait_send(fag, 15, 5)


def solution(mesh):
    def local_layer(x_in, seq_lens, k_cache, v_cache, ln1_gain, w_qkv, w_out, ln2_gain, w_up, w_down):
        any_spec = pl.BlockSpec(memory_space=pl.ANY)
        vmem = pl.BlockSpec(memory_space=pltpu.VMEM)
        x_out, k_new, v_new = pl.pallas_call(
            kernel,
            out_shape=(
                jax.ShapeDtypeStruct((BATCH, D), BF16),
                jax.ShapeDtypeStruct((BATCH, 16, 128), F32),
                jax.ShapeDtypeStruct((BATCH, 16, 128), F32),
            ),
            in_specs=[pl.BlockSpec(memory_space=pltpu.SMEM)] + [any_spec] * 9,
            out_specs=(vmem, vmem, vmem),
            scratch_shapes=[
                pltpu.VMEM((BATCH, D), BF16),
                pltpu.VMEM((1, D), F32),
                pltpu.VMEM((1, D), F32),
                pltpu.VMEM((N_CHUNKS, CHUNK, 16, 128), BF16),
                pltpu.VMEM((BATCH, 1024, 128), BF16),
                pltpu.VMEM((BATCH, 1024, 128), BF16),
                pltpu.VMEM((2048, D), BF16),
                pltpu.VMEM((D, FF_DEV), BF16),
                pltpu.VMEM((FF_DEV, D), BF16),
                pltpu.VMEM((32, 16, 2048), BF16),
                pltpu.VMEM((16, 8, 128), F32),
                pltpu.VMEM((16, 8, 128), F32),
                pltpu.VMEM((16, 8, 128), F32),
                pltpu.VMEM((64, 4, 128), F32),
                pltpu.VMEM((64, 4, 128), F32),
                pltpu.VMEM((2, 128), F32),
                pltpu.VMEM((64, 2, 128), F32),
                pltpu.VMEM((16, 8, 128), F32),
                pltpu.VMEM((BATCH, D), F32),
                pltpu.VMEM((BATCH, D), F32),
                pltpu.VMEM((16, 8, 256), F32),
                pltpu.VMEM((16, 8, 256), F32),
                pltpu.VMEM((16, 8, 256), F32),
                pltpu.VMEM((8, 256), F32),
                pltpu.VMEM((16, 8, 256), F32),
                pltpu.SemaphoreType.DMA((5,)),
                pltpu.SemaphoreType.DMA((N_CHUNKS,)),
                pltpu.SemaphoreType.DMA((3,)),
                pltpu.SemaphoreType.DMA((6,)),
                pltpu.SemaphoreType.DMA((6,)),
            ],
            compiler_params=pltpu.CompilerParams(
                collective_id=0, has_side_effects=True, vmem_limit_bytes=67043328),
            name="layer",
        )(
            seq_lens, x_in, ln1_gain.reshape(1, D), ln2_gain.reshape(1, D), w_qkv.reshape(D, 48, 128),
            k_cache.reshape(BATCH, 1024, 128), v_cache.reshape(BATCH, 1024, 128), w_out.reshape(2048, D), w_up, w_down,
        )
        slot_pos = lax.axis_index("sp") * TOK + jnp.arange(TOK)
        slot_hit = (slot_pos[None, :] == seq_lens[:, None])[:, :, None, None]
        k_next = jnp.where(slot_hit, k_new.astype(BF16)[:, None], k_cache)
        v_next = jnp.where(slot_hit, v_new.astype(BF16)[:, None], v_cache)
        return x_out, k_next, v_next

    cache_spec = P("dp", "sp", "tp", None)
    in_specs = (P("dp", None), P("dp"), cache_spec, cache_spec, P(None), P(None, None, "tp", None), P("tp", None, None), P(None), P(None, "tp"), P("tp", None))
    out_specs = (P("dp", None), cache_spec, cache_spec)
    return jax.shard_map(local_layer, mesh=mesh, in_specs=in_specs, out_specs=out_specs, check_vma=False)
```
